32 devices in a mesh: rep: 1 (over z), dp: 32 (over x, y, core).
Axes of the slice: x: 4, y: 4, z: 1, core: 2. Of those that a mesh axis runs over, the one named last changes fastest.
The devices are a block of a 4x4x8 slice.
Arguments:
- x: bfloat16 [32, 2048, 1024], P(('rep', 'dp'))
- dy: bfloat16 [32, 2048, 1024], P(('rep', 'dp'))
- w_gate: bfloat16 [2, 1024, 4096], replicated
- w_up: bfloat16 [2, 1024, 4096], replicated
- w_down: bfloat16 [2, 4096, 1024], replicated
- m_w_gate: float32 [2, 1024, 4096], P(None, 'dp')
- m_w_up: float32 [2, 1024, 4096], P(None, 'dp')
- m_w_down: float32 [2, 4096, 1024], P(None, 'dp')
- v_w_gate: float32 [2, 1024, 4096], P(None, 'dp')
- v_w_up: float32 [2, 1024, 4096], P(None, 'dp')
- v_w_down: float32 [2, 4096, 1024], P(None, 'dp')
Outputs:
- output 1: bfloat16 [2, 1024, 4096], P('rep')
- output 2: bfloat16 [2, 1024, 4096], P('rep')
- output 3: bfloat16 [2, 4096, 1024], P('rep')
- output 4: float32 [2, 1024, 4096], P('rep', 'dp')
- output 5: float32 [2, 1024, 4096], P('rep', 'dp')
- output 6: float32 [2, 4096, 1024], P('rep', 'dp')
- output 7: float32 [2, 1024, 4096], P('rep', 'dp')
- output 8: float32 [2, 1024, 4096], P('rep', 'dp')
- output 9: float32 [2, 4096, 1024], P('rep', 'dp')
All inputs are finite; a program needn't handle non-finite values.
Results may differ from the reference program's by a relative error of at most 0.022.
Values are sent between devices in bfloat16 or wider.
A program may use at most 768 MiB of HBM per device.

```python
import jax
import jax.numpy as jnp
from jax import lax

SEQUENCES = 32
TOKENS = 2048
D = 1024
FF = 4096
LAYERS = 2
NAMES = ("w_gate", "w_up", "w_down")
SHAPES = {"w_gate": (LAYERS, D, FF), "w_up": (LAYERS, D, FF), "w_down": (LAYERS, FF, D)}


def bump(key, n, height):
    away = (jnp.arange(n, dtype=jnp.int32) - jax.random.randint(key, (), 0, n, jnp.int32)) % n
    return jnp.where(away < n // 8, height, 1.0)


def together(key, own, strength):
    shared = jax.random.normal(key, own.shape[1:], jnp.float32)
    return (own + strength * shared) * lax.rsqrt(1 + strength * strength)


def setup_inputs(seed: int = 0, part: int = 0) -> dict:
    kx, kdy, ka, kb, kz, kf, kh, kl, *keys = jax.random.split(jax.random.key(seed), 8 + 3 * len(NAMES))
    kx, kdy, ka, kb = (jax.random.fold_in(k, part) for k in (kx, kdy, ka, kb))
    kw, km, kv = (keys[i::3] for i in range(3))
    shape = (SEQUENCES, TOKENS, D)
    much_x, much_dy = jax.random.uniform(kz, (2,), jnp.float32, 0.0, 1.0)
    loud = 2.0 ** jax.random.uniform(jax.random.fold_in(kz, 1), (), jnp.float32, -1.0, 2.0)
    layers = 2.0 ** jax.random.uniform(kl, (LAYERS, 1, 1), jnp.float32, -1.0, 1.0)
    x = together(ka, jax.random.normal(kx, shape, jnp.float32), much_x) * bump(kf, D, 4.0)
    dy = together(kb, jax.random.normal(kdy, shape, jnp.float32), much_dy)
    drawn = {"x": x.astype(jnp.bfloat16), "dy": (loud * dy * (SEQUENCES * TOKENS) ** -0.5).astype(jnp.bfloat16)}
    for key, name in zip(kw, NAMES, strict=True):
        w = jax.random.normal(key, SHAPES[name], jnp.float32) * SHAPES[name][1] ** -0.5
        drawn[name] = (w * {"w_gate": 1.0, "w_up": bump(kh, FF, 4.0), "w_down": layers}[name]).astype(jnp.bfloat16)
    for key, name in zip(km, NAMES, strict=True):
        drawn[f"m_{name}"] = 0.1 * jax.random.normal(key, SHAPES[name], jnp.float32)
    for key, name in zip(kv, NAMES, strict=True):
        drawn[f"v_{name}"] = jax.random.uniform(key, SHAPES[name], jnp.float32, 0.005, 0.015)
    return drawn


def matmul(a, w):
    return jnp.dot(a, w, preferred_element_type=jnp.float32).astype(jnp.bfloat16)


def normed(h):
    wide = h.astype(jnp.float32)
    scale = lax.rsqrt(jnp.mean(wide**2, -1, keepdims=True) + 1e-6)
    return (wide * scale).astype(jnp.bfloat16)


def layer(h, w):
    a = normed(h)
    gate = jnp.dot(a, w["w_gate"], preferred_element_type=jnp.float32)
    up = jnp.dot(a, w["w_up"], preferred_element_type=jnp.float32)
    return h + matmul((jax.nn.silu(gate) * up).astype(jnp.bfloat16), w["w_down"])


def adamw(w, m, v, g):
    m = 0.9 * m + 0.1 * g
    v = 0.95 * v + 0.05 * g * g
    step = m * lax.rsqrt(v + 1e-8) + 0.1 * w
    return (w - 0.02 * step).astype(jnp.bfloat16), m, v


def stack(weights, h):
    return lax.scan(lambda h, w: (layer(h, w), None), h, weights)[0]


def reference(x, dy, w_gate, w_up, w_down, m_w_gate, m_w_up, m_w_down, v_w_gate, v_w_up, v_w_down):
    weights = dict(zip(NAMES, (w_gate, w_up, w_down), strict=True))

    def take(so_far, sequence):
        h, by_y = sequence
        _, back = jax.vjp(lambda w: stack(w, h), weights)
        return jax.tree.map(lambda total, term: total + term.astype(jnp.float32), so_far, back(by_y)[0]), None

    none_yet = {name: jnp.zeros(w.shape, jnp.float32) for name, w in weights.items()}
    by_weights, _ = lax.scan(take, none_yet, (x, dy))
    gradients = [by_weights[name].astype(jnp.bfloat16).astype(jnp.float32) for name in NAMES]
    new = [
        adamw(w.astype(jnp.float32), m, v, g)
        for w, m, v, g in zip((w_gate, w_up, w_down), (m_w_gate, m_w_up, m_w_down), (v_w_gate, v_w_up, v_w_down), gradients, strict=True)
    ]
    return tuple(one[which] for which in range(3) for one in new)
```

```python
import functools
import jax, jax.numpy as jnp
from jax import lax
from jax.experimental import pallas as pl
from jax.experimental.pallas import tpu as pltpu
bf=jnp.bfloat16; f32=jnp.float32
VM=62*2**20
def dot(a,b): return jnp.dot(a,b,preferred_element_type=f32)
def dot_nt(a,b): return lax.dot_general(a,b,(((1,),(1,)),((),())),preferred_element_type=f32)
def normed(h):
    wide=h.astype(f32)
    return (wide*lax.rsqrt(jnp.mean(wide**2,-1,keepdims=True)+1e-6)).astype(bf)

def p0(x,wg,wu,tm=1024,tf=512,rm=256,rf=256):
    T,Dm=x.shape; F=wg.shape[-1]
    def kern(x_ref,wg_ref,wu_ref,hid_ref,hidT_ref,s_ref,t_ref,aT_ref,a_sc):
        f=pl.program_id(0); t=pl.program_id(1)
        @pl.when(f==0)
        def _():
            a=normed(x_ref[...])
            a_sc[pl.ds(pl.multiple_of(t*tm,tm),tm),:]=a
            aT_ref[...]=a.T
        for r in range(tm//rm):
            a=a_sc[pl.ds(pl.multiple_of(t*tm+r*rm,rm),rm),:]
            for c in range(tf//rf):
                cs=slice(c*rf,(c+1)*rf); rs=slice(r*rm,(r+1)*rm)
                gate=dot(a,wg_ref[0,:,cs]); up=dot(a,wu_ref[0,:,cs])
                sg=jax.nn.sigmoid(gate); s=gate*sg
                s_ref[rs,cs]=s
                t_ref[rs,cs]=up*(sg*(1.0+gate*(1.0-sg)))
                hid=(s*up).astype(bf)
                hid_ref[rs,cs]=hid
                hidT_ref[cs,rs]=hid.T
    nt=T//tm; last=nt-1
    return pl.pallas_call(kern,grid=(F//tf,nt),
        in_specs=[pl.BlockSpec((tm,Dm),lambda f,t:(jnp.where(f==0,t,last),0)),
                  pl.BlockSpec((1,Dm,tf),lambda f,t:(0,0,f)),pl.BlockSpec((1,Dm,tf),lambda f,t:(0,0,f))],
        out_specs=[pl.BlockSpec((tm,tf),lambda f,t:(t,f)),pl.BlockSpec((tf,tm),lambda f,t:(f,t)),
                   pl.BlockSpec((tm,tf),lambda f,t:(t,f)),pl.BlockSpec((tm,tf),lambda f,t:(t,f)),
                   pl.BlockSpec((Dm,tm),lambda f,t:(0,jnp.where(f==0,t,last)))],
        out_shape=[jax.ShapeDtypeStruct((T,F),bf),jax.ShapeDtypeStruct((F,T),bf),jax.ShapeDtypeStruct((T,F),f32),jax.ShapeDtypeStruct((T,F),f32),jax.ShapeDtypeStruct((Dm,T),bf)],
        scratch_shapes=[pltpu.VMEM((T,Dm),bf)],
        compiler_params=pltpu.CompilerParams(vmem_limit_bytes=VM,dimension_semantics=("arbitrary","arbitrary")),name="p0")(x,wg,wu)

def p1(x,hid,wd,tm=512):
    T,Dm=x.shape; F=hid.shape[1]
    def kern(x_ref,hid_ref,wd_ref,h_ref,a_ref,aT_ref):
        for r in range(tm//256):
            rs=slice(r*256,(r+1)*256)
            y=dot(hid_ref[rs,:],wd_ref[0]).astype(bf)
            h=x_ref[rs,:]+y
            h_ref[rs,:]=h
            a=normed(h)
            a_ref[rs,:]=a
            aT_ref[:,rs]=a.T
    return pl.pallas_call(kern,grid=(T//tm,),
        in_specs=[pl.BlockSpec((tm,Dm),lambda t:(t,0)),pl.BlockSpec((tm,F),lambda t:(t,0)),pl.BlockSpec((1,F,Dm),lambda t:(0,0,0))],
        out_specs=[pl.BlockSpec((tm,Dm),lambda t:(t,0)),pl.BlockSpec((tm,Dm),lambda t:(t,0)),pl.BlockSpec((Dm,tm),lambda t:(0,t))],
        out_shape=[jax.ShapeDtypeStruct((T,Dm),bf),jax.ShapeDtypeStruct((T,Dm),bf),jax.ShapeDtypeStruct((Dm,T),bf)],
        compiler_params=pltpu.CompilerParams(vmem_limit_bytes=VM),name="p1")(x,hid,wd)

def p2(a,dy,wg,wu,wd,layer,tm=1024,tf=512,rm=256,rf=256):
    T,Dm=a.shape; F=wg.shape[-1]
    def kern(a_ref,dy_ref,wg_ref,wu_ref,wd_ref,hidT_ref,dg_ref,du_ref):
        t=pl.program_id(1)
        for r in range(tm//rm):
            ro=pl.ds(pl.multiple_of(t*tm+r*rm,rm),rm)
            av=a_ref[ro,:]; dv=dy_ref[ro,:]
            for c in range(tf//rf):
                cs=slice(c*rf,(c+1)*rf); rs=slice(r*rm,(r+1)*rm)
                gate=dot(av,wg_ref[0,:,cs]); up=dot(av,wu_ref[0,:,cs])
                dh=dot_nt(dv,wd_ref[0,cs,:]).astype(bf).astype(f32)
                sg=jax.nn.sigmoid(gate); s=gate*sg
                du_ref[rs,cs]=(dh*s).astype(bf)
                dg_ref[rs,cs]=(dh*(up*(sg*(1.0+gate*(1.0-sg))))).astype(bf)
                hidT_ref[cs,rs]=(s*up).astype(bf).T
    return pl.pallas_call(kern,grid=(F//tf,T//tm),
        in_specs=[pl.BlockSpec((T,Dm),lambda f,t:(0,0)),pl.BlockSpec((T,Dm),lambda f,t:(0,0)),
                  pl.BlockSpec((1,Dm,tf),lambda f,t:(layer,0,f)),pl.BlockSpec((1,Dm,tf),lambda f,t:(layer,0,f)),pl.BlockSpec((1,tf,Dm),lambda f,t:(layer,f,0))],
        out_specs=[pl.BlockSpec((tf,tm),lambda f,t:(f,t)),pl.BlockSpec((tm,tf),lambda f,t:(t,f)),pl.BlockSpec((tm,tf),lambda f,t:(t,f))],
        out_shape=[jax.ShapeDtypeStruct((F,T),bf),jax.ShapeDtypeStruct((T,F),bf),jax.ShapeDtypeStruct((T,F),bf)],
        compiler_params=pltpu.CompilerParams(vmem_limit_bytes=VM),name="p2")(a,dy,wg,wu,wd)
import math
MESH=pl.DeviceIdType.MESH
div,rem=lax.div,lax.rem

def mega(n,hid1T,a1T,hid0T,a0T,dy,dg1,du1,wg,wu,wd,s0,t0,h1,mg,mu,md,vg,vu,vd,axis="dp"):
    T,Dm=dy.shape; L,_,F=wg.shape
    S=math.isqrt(n//2); R=Dm//n; Q=Dm//4; K=F//Dm
    assert S==4 and 2*S*S==n and F==4*Dm and L==2 and R%16==0 and Q%128==0
    U=3*L*K; N=U+8; TM=T//4
    hv=lambda h: h.reshape(S,S,2,K,R,T)
    av=lambda a: a.reshape(S,S,2,R,T)
    def kern(hid1T,a1T,hid0T,a0T,dy,dg1,du1,wg,wu,wd,s0,t0,h1,mg,mu,md,vg,vu,vd,
             wag,gsum,dg0,du0,
             lhs,rhs,own,dsend,drecv,r1,r2,r3,e1,e2,e3,pf,q1,q2,q3,x1,x2,x3,wst,win,min_,vin,gst,
             wbuf,gt,ut,ht,yt,st,tt,
             lsem,rsem,wsem,gsem,ssem,osem,isem,nsem,csem,
             dss,drs,ss,rs,ads,adr):
        me=lax.axis_index(axis)
        c=rem(me,2); y=rem(div(me,2),S); x=div(me,2*S)
        idx=lambda x,y,c: (rem(x+S,S)*S+rem(y+S,S))*2+c
        nb=[idx(x+1,y,c),idx(x-1,y,c),idx(x,y+1,c),idx(x,y-1,c)]; pa=idx(x,y,1-c)
        bar=pltpu.get_barrier_semaphore()
        for d in nb+[pa]:
            pl.semaphore_signal(bar,inc=1,device_id={axis:d},device_id_type=MESH)
        pl.semaphore_wait(bar,5)
        AB=[(x,y),(y,x)]
        P1=[(0,1),(2,3)]; P2=[(2,3),(0,1)]
        def rc(src,dst,s,r,dev):
            return pltpu.make_async_remote_copy(src_ref=src,dst_ref=dst,send_sem=s,recv_sem=r,device_id={axis:dev},device_id_type=MESH)
        cp=pltpu.make_async_copy
        def jk(u):
            l,v=div(u,3*K),rem(u,3*K); w=v-K
            return 3*l+jnp.where(v<K,0,1+rem(w,2)),jnp.where(v<K,v,div(w,2))
        def loc(u): j,k=jk(u); return j*K+k
        two=lambda u: rem(u,2)
        four=lambda u: rem(u,4)
        def sems(kind,u,d): return ss.at[kind,two(u),d],rs.at[kind,four(u),d],nb[d]
        m1,m2,m3,o1,o2,o3=(lambda u,d,kind=kind,e=e,r=r: rc(e.at[two(u),d],r.at[four(u),d],*sems(kind,u,d))
                           for kind,(e,r) in enumerate(((e1,r1),(e2,r2),(e3,r3),(x1,q1),(x2,q2),(x3,q3))))
        pair=lambda g: pl.ds(2*g,2)
        up_,down_=(lambda v: rem(v+1,S)),(lambda v: rem(v+S-1,S))
        behind=lambda v,s: (down_,up_)[s](v)
        far_=lambda v: rem(v+2,S)
        def g1(u,g,s):
            a,b=AB[g]; d=P2[g][s]
            return rc(wst.at[two(u),pair(g)],wag.at[loc(u),c,pair(g),a,b],*sems(6,u,d))
        def g2(u,g,s):
            a,b=AB[g]; d=P2[g][s]; r=wag.at[loc(u),c,2*g+s,a,behind(b,s)]
            return rc(r,r,*sems(7,u,d))
        def g3(u,g,s):
            a,b=AB[g]; d=P1[g][s]; r=wag.at[loc(u),c,pair(g),a]
            return rc(r,r,*sems(8,u,d))
        def g4(u,g,s):
            a,b=AB[g]; d=P1[g][s]; r=wag.at[loc(u),c,2*g+s,behind(a,s)]
            return rc(r,r,*sems(9,u,d))
        def d2(u): return rc(dsend,drecv.at[four(u)],dss,drs.at[four(u)],pa)
        def gd(u): return rc(wag.at[loc(u),c],wag.at[loc(u),c],ads.at[two(u)],adr.at[four(u)],pa)
        GS=[(g,s) for g in range(2) for s in range(2)]
        f=lambda v: v.astype(f32)
        def lhs_load(u,h):
            j,k=jk(u); cc=(1-c) if h else c; dst=lhs.at[h]; sem=lsem.at[h]
            @pl.when(j==0)
            def _(): cp(hid1T.at[:,:,cc,k],dst,sem).start()
            @pl.when(u==K)
            def _(): cp(a1T.at[:,:,cc],dst,sem).start()
            @pl.when(j==3)
            def _(): cp(hid0T.at[:,:,cc,k],dst,sem).start()
            @pl.when(u==4*K)
            def _(): cp(a0T.at[:,:,cc],dst,sem).start()
        def lhs_wait(u,h):
            @pl.when(rem(u,3*K)<=K)
            def _(): cp(a1T.at[:,:,c],lhs.at[h],lsem.at[h]).wait()
        def rhs_load(u):
            j,k=jk(u); dst=rhs.at[0]; sem=rsem; cols=pl.ds(pl.multiple_of(k*Dm,Dm),Dm)
            @pl.when(u==0)
            def _(): cp(dy,dst,sem).start()
            @pl.when(j==1)
            def _(): cp(dg1.at[:,cols],dst,sem).start()
            @pl.when(j==2)
            def _(): cp(du1.at[:,cols],dst,sem).start()
            @pl.when(j==4)
            def _(): cp(dg0.at[:,cols],dst,sem).start()
            @pl.when(j==5)
            def _(): cp(du0.at[:,cols],dst,sem).start()
        def rhs_wait(u):
            @pl.when((u==0)|(rem(u,3*K)>=K))
            def _(): cp(dy,rhs.at[0],rsem).wait()
        def state(u,go):
            j,k=jk(u); l=1-div(j,3); t=rem(j,3); sl=two(u)
            cols=pl.ds(pl.multiple_of(k*Dm,Dm),Dm)
            def three(mr,vr,wr):
                go(cp(mr,min_.at[sl],isem.at[0,sl])); go(cp(vr,vin.at[sl],isem.at[1,sl])); go(cp(wr,win.at[sl],isem.at[2,sl]))
            @pl.when(t==0)
            def _():
                r=pl.ds(pl.multiple_of(k*R,R),R)
                three(md.at[l,r],vd.at[l,r],wd.at[l,pl.ds(pl.multiple_of(me*(K*R)+k*R,R),R)])
            @pl.when(t==1)
            def _(): three(mg.at[l,:,cols],vg.at[l,:,cols],wg.at[l,pl.ds(pl.multiple_of(me*R,R),R),cols])
            @pl.when(t==2)
            def _(): three(mu.at[l,:,cols],vu.at[l,:,cols],wu.at[l,pl.ds(pl.multiple_of(me*R,R),R),cols])
        start=lambda d: d.start()
        wait=lambda d: d.wait()
        def both(q,o,u): return f(own[rem(u,3),q,o])+f(drecv[four(u),q,o])
        def at(i,dl,body):
            u=i-dl
            @pl.when((u>=0)&(u<U))
            def _(): body(u)
        def sA1(u):
            d2(u).wait()
            sl=four(u); w=two(u)
            for g in range(2):
                a,b=AB[g]; p,m=P1[g]
                far=far_(a)
                e1[w,p]=both(2*g,far,u).astype(bf); m1(u,p).start()
                e1[w,m]=both(2*g+1,far,u).astype(bf); m1(u,m).start()
            for g in range(2):
                a,b=AB[g]; p,m=P1[g]
                e2[w,p]=both(2*g+1,up_(a),u).astype(bf); m2(u,p).start()
                e2[w,m]=both(2*g,down_(a),u).astype(bf); m2(u,m).start()
        def sA2(u):
            sl=four(u); w=two(u)
            for d in range(4): m1(u,d).wait_send(); m2(u,d).wait_send()
            for g in range(2):
                a,b=AB[g]; p,m=P1[g]
                m1(u,p).wait_recv()
                e3[w,p]=(both(2*g,up_(a),u)+f(r1[sl,p])).astype(bf); m3(u,p).start()
                m1(u,m).wait_recv()
                e3[w,m]=(both(2*g+1,down_(a),u)+f(r1[sl,m])).astype(bf); m3(u,m).start()
        def sA3(u):
            sl=four(u); w=two(u)
            for d in range(4): m3(u,d).wait_send()
            for g in range(2):
                a,b=AB[g]; p,m=P1[g]
                for d in (p,m): m2(u,d).wait_recv(); m3(u,d).wait_recv()
                pf[w,2*g]=both(2*g,a,u)+f(r3[sl,p])+f(r2[sl,m])
                pf[w,2*g+1]=both(2*g+1,a,u)+f(r2[sl,p])+f(r3[sl,m])
                p,m=P2[g]; far=far_(b)
                x1[w,p]=pf[w,2*g,far].astype(bf); o1(u,p).start()
                x1[w,m]=pf[w,2*g+1,far].astype(bf); o1(u,m).start()
                x2[w,p]=pf[w,2*g+1,up_(b)].astype(bf); o2(u,p).start()
                x2[w,m]=pf[w,2*g,down_(b)].astype(bf); o2(u,m).start()
        def sB3(u):
            sl=four(u); w=two(u)
            for g in range(2):
                a,b=AB[g]; p,m=P2[g]
                o1(u,p).wait_recv()
                x3[w,p]=(pf[w,2*g,up_(b)]+f(q1[sl,p])).astype(bf); o3(u,p).start()
                o1(u,m).wait_recv()
                x3[w,m]=(pf[w,2*g+1,down_(b)]+f(q1[sl,m])).astype(bf); o3(u,m).start()
            for d in range(4): o1(u,d).wait_send(); o2(u,d).wait_send()
        def sA4(u):
            sl=four(u); w=two(u)
            state(u,wait)
            for d in range(4): o3(u,d).wait_send()
            for g in range(2):
                a,b=AB[g]; p,m=P2[g]
                for d in (p,m): o2(u,d).wait_recv(); o3(u,d).wait_recv()
                for h in range(2):
                    q=2*g+h
                    tot=pf[w,q,b]+(f(q3[sl,p])+f(q2[sl,m]) if h==0 else f(q2[sl,p])+f(q3[sl,m]))
                    gr=f(tot.astype(bf)); cs=slice(q*Q,(q+1)*Q)
                    mn=0.9*min_[w,:,cs]+0.1*gr
                    vn=0.95*vin[w,:,cs]+0.05*gr*gr
                    wo=f(win[w,:,cs])
                    wst[w,q]=(wo-0.02*(mn*lax.rsqrt(vn+1e-8)+0.1*wo)).astype(bf)
                    gst[w,:,cs]=gr.astype(bf)
                for s in range(2): g1(u,g,s).start()
                cp(wst.at[w,pair(g)],wag.at[loc(u),c,pair(g),a,b],csem.at[w,g]).start()
            cp(gst.at[w],gsum.at[loc(u)],nsem.at[w]).start()
        def sB4(u):
            for g,s in GS:
                g1(u,g,s).wait_recv(); g2(u,g,s).start()
        def sB5(u):
            w=rem(u,2)
            for g,s in GS:
                g1(u,g,s).wait_send(); g2(u,g,s).wait_send()
            for g in range(2):
                a,b=AB[g]
                cp(wst.at[w,pair(g)],wag.at[loc(u),c,pair(g),a,b],csem.at[w,g]).wait()
                for s in range(2): g2(u,g,s).wait_recv()
                for s in range(2): g3(u,g,s).start()
            cp(gst.at[w],gsum.at[loc(u)],nsem.at[w]).wait()
        def sB6(u):
            for g,s in GS: g3(u,g,s).wait_send()
            for g,s in GS:
                g3(u,g,s).wait_recv(); g4(u,g,s).start()
        def sB7(u):
            for g,s in GS: g4(u,g,s).wait()
            gd(u).start()
        def sB8(u): gd(u).wait()
        def part(u,h):
            lhs_wait(u,h)
            rsl=jnp.where(jk(u)[0]==3,1,0)
            for q in range(4):
                o=dot(lhs[h].reshape(S*S*R,T),rhs[rsl,:,q*Q:(q+1)*Q]).astype(bf)
                for A in range(S):
                    for B in range(S):
                        blk=o[(A*S+B)*R:(A*S+B+1)*R]
                        o_,i_=(A,B) if q<2 else (B,A)
                        if h: dsend[q,o_,i_]=blk
                        else: own[rem(u,3),q,o_,i_]=blk
            @pl.when(u+1<U)
            def _(): lhs_load(u+1,h)
        tiles=lambda r: pl.ds(pl.multiple_of(r*TM,TM),TM)
        def da_load(v):
            r,h=div(v,2),rem(v,2); rr=tiles(r)
            @pl.when(h==0)
            def _(): cp(du1.at[rr],gt,gsem.at[0]).start()
            @pl.when(h==1)
            def _():
                cp(dg1.at[rr],gt,gsem.at[0]).start()
                cp(h1.at[rr],ht,gsem.at[1]).start(); cp(dy.at[rr],yt,gsem.at[2]).start()
        def w1_load(): return [cp(wu.at[1],wbuf.at[0],wsem.at[0]),cp(wg.at[1],wbuf.at[1],wsem.at[1])]
        def wd_load(): return [cp(wd.at[0,pl.ds(k*Dm,Dm)],wbuf.at[0,:,pl.ds(k*Dm,Dm)],wsem.at[2+k]) for k in range(K)]
        def da_slice(v):
            r,h=div(v,2),rem(v,2); rr=tiles(r)
            @pl.when(v==0)
            def _():
                for d in w1_load(): d.wait()
            cp(du1.at[rr],gt,gsem.at[0]).wait()
            da=dot_nt(gt[...],wbuf[h]).astype(bf)
            @pl.when(h==0)
            def _(): ut[...]=da
            @pl.when(h==1)
            def _():
                cp(h1.at[rr],ht,gsem.at[1]).wait(); cp(dy.at[rr],yt,gsem.at[2]).wait()
                db=f((f(da)+f(ut[...])).astype(bf))
                wide=f(ht[...])
                sc=lax.rsqrt(jnp.mean(wide*wide,-1,keepdims=True)+1e-6)
                dn=db*sc-wide*(sc*sc*sc*jnp.mean(db*wide,-1,keepdims=True))
                rhs[1,rr,:]=(f(yt[...])+f(dn.astype(bf))).astype(bf)
            @pl.when(v<7)
            def _(): da_load(v+1)
            @pl.when(v==7)
            def _():
                for d in wd_load(): d.start()
                for r in (0,1):
                    for d in st_load(0,r): d.start()
        HC=Dm//2
        def st_load(v,r):
            cc=pl.ds(pl.multiple_of(v*HC,HC),HC); rr=pl.ds(r*TM,TM); sl=r%2
            return [cp(s0.at[rr,cc],st.at[sl],ssem.at[0,sl]),cp(t0.at[rr,cc],tt.at[sl],ssem.at[1,sl])]
        def put(v,r):
            cc=pl.ds(pl.multiple_of(v*HC,HC),HC); rr=pl.ds(r*TM,TM)
            return [cp(gt.at[:,pl.ds((2*r+h)*HC,HC)],o.at[rr,cc],osem.at[h,r]) for h,o in enumerate((dg0,du0))]
        def dh_slice(v,rs):
            k=div(v,2); w=wbuf[0,pl.ds(pl.multiple_of(rem(v,2)*HC,HC),HC),pl.ds(pl.multiple_of(k*Dm,Dm),Dm)]
            for r in rs:
                for d in st_load(v,r): d.wait()
                dh=f(dot_nt(rhs[1,r*TM:(r+1)*TM,:],w).astype(bf))
                gt[:,(2*r)*HC:(2*r+1)*HC]=(dh*tt[r%2]).astype(bf)
                gt[:,(2*r+1)*HC:(2*r+2)*HC]=(dh*st[r%2]).astype(bf)
                for d in put(v,r): d.start()
        def dh_first(v):
            @pl.when(v==0)
            def _():
                for d in wd_load(): d.wait()
            @pl.when(v>0)
            def _():
                for r in (2,3):
                    for d in put(v-1,r): d.wait()
            dh_slice(v,(0,1))
            for r in (2,3):
                for d in st_load(v,r): d.start()
        def dh_second(v):
            dh_slice(v,(2,3))
            for r in (0,1):
                for d in put(v,r): d.wait()
            @pl.when(v<2*K-1)
            def _():
                for r in (0,1):
                    for d in st_load(v+1,r): d.start()
            @pl.when(v==2*K-1)
            def _():
                for r in (2,3):
                    for d in put(v,r): d.wait()
        lhs_load(0,1); rhs_load(0); lhs_load(0,0)
        da_load(0)
        for d in w1_load(): d.start()
        @pl.loop(0,N)
        def _(i):
            at(i,4,sA4); at(i,3,sA3); at(i,2,sA2); at(i,1,sA1)
            @pl.when(i<U)
            def _():
                rhs_wait(i)
                part(i,1)
                d2(i).start()
            at(i,3,sB3); at(i,4,sB4); at(i,5,sB5); at(i,6,sB6); at(i,7,sB7); at(i,8,sB8)
            at(i,3,lambda u: state(u,start))
            @pl.when((i>=12)&(i<12+2*K))
            def _(): dh_first(i-12)
            @pl.when(i<U)
            def _():
                part(i,0)
                @pl.when(i+1<U)
                def _(): rhs_load(i+1)
            @pl.when((i>=4)&(i<12))
            def _(): da_slice(i-4)
            @pl.when((i>=12)&(i<12+2*K))
            def _(): dh_second(i-12)
    A=pl.BlockSpec(memory_space=pl.ANY)
    sd=jax.ShapeDtypeStruct
    V=pltpu.VMEM; DS=pltpu.SemaphoreType.DMA
    msg=lambda k: V((k,4,S,R,Q),bf)
    small=lambda k: V((k,4,R,Q),bf)
    out=pl.pallas_call(kern,
        in_specs=[A]*19,out_specs=[A]*4,
        out_shape=[sd((U,2,4,S,S,R,Q),bf)]+[sd((U,R,Dm),bf)]+[sd((T,F),bf)]*2,
        scratch_shapes=[V((2,S,S,R,T),bf),V((2,T,Dm),bf),V((3,4,S,S,R,Q),bf),V((4,S,S,R,Q),bf),V((4,4,S,S,R,Q),bf),
            msg(4),msg(4),msg(4),msg(2),msg(2),msg(2),V((2,4,S,R,Q),f32),
            small(4),small(4),small(4),small(2),small(2),small(2),
            V((2,4,R,Q),bf),V((2,R,Dm),bf),V((2,R,Dm),f32),V((2,R,Dm),f32),V((2,R,Dm),bf),
            V((2,Dm,F),bf),V((TM,F),bf),V((TM,Dm),bf),V((TM,Dm),bf),V((TM,Dm),bf),V((2,TM,Dm//2),f32),V((2,TM,Dm//2),f32),
            DS((2,)),DS(()),DS((2+K,)),DS((3,)),DS((2,2)),DS((2,4)),DS((3,2)),DS((2,)),DS((2,2)),
            DS(()),DS((4,)),DS((10,2,4)),DS((10,4,4)),DS((2,)),DS((4,))],
        compiler_params=pltpu.CompilerParams(collective_id=0,has_side_effects=True,vmem_limit_bytes=67043328),name="mega",
    )(hv(hid1T),av(a1T),hv(hid0T),av(a0T),dy,dg1,du1,wg,wu,wd,s0,t0,h1,mg,mu,md,vg,vu,vd)
    return out

def final(wag,gsum,ms,vs):
    U,_,_,S,_,R,Q=wag.shape; n=2*S*S; Dm=4*Q; L=ms[0].shape[0]; K=U//(3*L)
    ms=(ms[0].reshape(L,K,R,Dm),*ms[1:]); vs=(vs[0].reshape(L,K,R,Dm),*vs[1:])
    B=2
    def kern(w_ref,g_ref,*refs):
        m,v,wo,mo,vo=(refs[3*i:3*i+3] for i in range(5))
        kind=div(B*pl.program_id(0),L*K)
        for t in range(3):
            @pl.when(kind==t)
            def _():
                for p in range(B):
                    for cc in range(2):
                        for r in range(S*S):
                            for q in range(4):
                                v_=w_ref[p,cc,q,r//S,r%S] if q<2 else w_ref[p,cc,q,r%S,r//S]
                                if t: wo[t][0,(2*r+cc)*R:(2*r+cc+1)*R,p*Dm+q*Q:p*Dm+q*Q+Q]=v_
                                else: wo[t][0,2*r+cc,p,:,q*Q:q*Q+Q]=v_
                    g=g_ref[p].astype(f32)
                    at=(0,slice(None),slice(p*Dm,p*Dm+Dm)) if t else (0,p)
                    mo[t][at]=0.9*m[t][at]+0.1*g
                    vo[t][at]=0.95*v[t][at]+0.05*g*g
    H=K//B; E=L*H
    def lk(s,t): s=jnp.clip(s-t*E,0,E-1); return div(s,H),rem(s,H)
    def unit(s): l,k=lk(rem(s,E),0); return ((L-1-l)*3+div(s,E))*H+k
    def spec(t,d,g):
        def at(s): l,k=lk(s,t); return (l,0,k) if t else (l,*[0]*(len(d)-4),k,0,0)
        return pl.BlockSpec(g if t else d,at)
    sd=jax.ShapeDtypeStruct
    mom=[spec(t,(1,B,R,Dm),(1,R,B*Dm)) for t in range(3)]
    o=pl.pallas_call(kern,grid=(U//B,),
        in_specs=[pl.BlockSpec((B,2,4,S,S,R,Q),lambda s:(unit(s),*[0]*6)),pl.BlockSpec((B,R,Dm),lambda s:(unit(s),0,0))]+mom*2,
        out_specs=[spec(t,(1,n,B,R,Dm),(1,Dm,B*Dm)) for t in range(3)]+mom*2,
        out_shape=[sd((L,n,K,R,Dm),bf),sd((L,Dm,K*Dm),bf),sd((L,Dm,K*Dm),bf)]+[sd(a.shape,f32) for a in (*ms,*vs)],
        name="final",compiler_params=pltpu.CompilerParams(vmem_limit_bytes=VM))(wag,gsum,*ms,*vs)
    w,m,v=o[:3],o[3:6],o[6:]
    order=lambda d,g,u: (g,u,d.reshape(L,-1,Dm))
    return (*order(*w),*order(*m),*order(*v))

def solution(mesh):
    from jax.sharding import PartitionSpec as P
    n=mesh.shape["dp"]
    def step(x,dy,wg,wu,wd,mg,mu,md,vg,vu,vd):
        x,dy=x[0],dy[0]
        hid0,hid0T,s0,t0,a0T=p0(x,wg,wu)
        h1,a1,a1T=p1(x,hid0,wd)
        hid1T,dg1,du1=p2(a1,dy,wg,wu,wd,1)
        wag,gsum,_,_=mega(n,hid1T,a1T,hid0T,a0T,dy,dg1,du1,wg,wu,wd,s0,t0,h1,mg,mu,md,vg,vu,vd)
        return final(wag,gsum,(md,mg,mu),(vd,vg,vu))
    tok=P(("rep","dp"),None,None); w=P(None,None,None); m=P(None,"dp",None)
    return jax.shard_map(step,mesh=mesh,in_specs=(tok,tok,w,w,w)+(m,)*6,
        out_specs=(P("rep",None,None),)*3+(P("rep","dp",None),)*6,check_vma=False)
```

```python
import functools
import jax, jax.numpy as jnp
from jax import lax
from jax.experimental import pallas as pl
from jax.experimental.pallas import tpu as pltpu
bf=jnp.bfloat16; f32=jnp.float32
VM=62*2**20
def dot(a,b): return jnp.dot(a,b,preferred_element_type=f32)
def dot_nt(a,b): return lax.dot_general(a,b,(((1,),(1,)),((),())),preferred_element_type=f32)
def normed(h):
    wide=h.astype(f32)
    return (wide*lax.rsqrt(jnp.mean(wide**2,-1,keepdims=True)+1e-6)).astype(bf)

def p01(x,wg,wu,wd,tm=512,tf=1024,rm=256,rf=256):
    T,Dm=x.shape; F=wg.shape[-1]; nf=F//tf
    def kern(x_ref,wg,wu,wd,hidT_ref,s_ref,t_ref,aT_ref,h_ref,a_ref,a1T_ref,gs,us,ds,a_sc,hid_sc,acc,sem):
        t,f=pl.program_id(0),pl.program_id(1)
        part=lambda f: pl.ds(pl.multiple_of(f*tf,tf),tf)
        def loads(f):
            p=part(f)
            return [pltpu.make_async_copy(a,b,sem.at[i,f]) for i,(a,b) in enumerate(((wg.at[0,:,p],gs.at[:,p]),(wu.at[0,:,p],us.at[:,p]),(wd.at[0,p],ds.at[p])))]
        @pl.when((t==0)&(f==0))
        def _():
            for g in range(nf):
                for d in loads(g): d.start()
        @pl.when(f==0)
        def _():
            a=normed(x_ref[...])
            a_sc[...]=a
            aT_ref[...]=a.T
            acc[...]=jnp.zeros_like(acc)
        @pl.when(t==0)
        def _():
            for d in loads(f): d.wait()
        for r in range(tm//rm):
            rs=slice(r*rm,(r+1)*rm); a=a_sc[rs,:]
            for c in range(tf//rf):
                cs=slice(c*rf,(c+1)*rf); cols=pl.ds(pl.multiple_of(f*tf+c*rf,rf),rf)
                gate=dot(a,gs[:,cols]); up=dot(a,us[:,cols])
                sg=jax.nn.sigmoid(gate); s=gate*sg
                s_ref[rs,cs]=s
                t_ref[rs,cs]=up*(sg*(1.0+gate*(1.0-sg)))
                hid=(s*up).astype(bf)
                hid_sc[rs,cs]=hid
                hidT_ref[cs,rs]=hid.T
        acc[...]+=dot(hid_sc[...],ds[part(f),:])
        @pl.when(f==nf-1)
        def _():
            h=x_ref[...]+acc[...].astype(bf)
            h_ref[...]=h
            a=normed(h)
            a_ref[...]=a
            a1T_ref[...]=a.T
    A=pl.BlockSpec(memory_space=pl.ANY)
    row=pl.BlockSpec((tm,Dm),lambda t,f:(t,0)); col=pl.BlockSpec((Dm,tm),lambda t,f:(0,t)); tile=pl.BlockSpec((tm,tf),lambda t,f:(t,f))
    sd=jax.ShapeDtypeStruct; V=pltpu.VMEM
    return pl.pallas_call(kern,grid=(T//tm,nf),in_specs=[row,A,A,A],
        out_specs=[pl.BlockSpec((tf,tm),lambda t,f:(f,t)),tile,tile,col,row,row,col],
        out_shape=[sd((F,T),bf),sd((T,F),f32),sd((T,F),f32),sd((Dm,T),bf),sd((T,Dm),bf),sd((T,Dm),bf),sd((Dm,T),bf)],
        scratch_shapes=[V((Dm,F),bf),V((Dm,F),bf),V((F,Dm),bf),V((tm,Dm),bf),V((tm,tf),bf),V((tm,Dm),f32),pltpu.SemaphoreType.DMA((3,nf))],
        compiler_params=pltpu.CompilerParams(vmem_limit_bytes=VM),name="p01")(x,wg,wu,wd)

def p2(a,dy,wg,wu,wd,layer,tm=1024,tf=512,rm=256,rf=256):
    T,Dm=a.shape; F=wg.shape[-1]
    def kern(a_ref,dy_ref,wg_ref,wu_ref,wd_ref,hidT_ref,dg_ref,du_ref):
        t=pl.program_id(1)
        for r in range(tm//rm):
            ro=pl.ds(pl.multiple_of(t*tm+r*rm,rm),rm)
            av=a_ref[ro,:]; dv=dy_ref[ro,:]
            for c in range(tf//rf):
                cs=slice(c*rf,(c+1)*rf); rs=slice(r*rm,(r+1)*rm)
                gate=dot(av,wg_ref[0,:,cs]); up=dot(av,wu_ref[0,:,cs])
                dh=dot_nt(dv,wd_ref[0,cs,:]).astype(bf).astype(f32)
                sg=jax.nn.sigmoid(gate); s=gate*sg
                du_ref[rs,cs]=(dh*s).astype(bf)
                dg_ref[rs,cs]=(dh*(up*(sg*(1.0+gate*(1.0-sg))))).astype(bf)
                hidT_ref[cs,rs]=(s*up).astype(bf).T
    return pl.pallas_call(kern,grid=(F//tf,T//tm),
        in_specs=[pl.BlockSpec((T,Dm),lambda f,t:(0,0)),pl.BlockSpec((T,Dm),lambda f,t:(0,0)),
                  pl.BlockSpec((1,Dm,tf),lambda f,t:(layer,0,f)),pl.BlockSpec((1,Dm,tf),lambda f,t:(layer,0,f)),pl.BlockSpec((1,tf,Dm),lambda f,t:(layer,f,0))],
        out_specs=[pl.BlockSpec((tf,tm),lambda f,t:(f,t)),pl.BlockSpec((tm,tf),lambda f,t:(t,f)),pl.BlockSpec((tm,tf),lambda f,t:(t,f))],
        out_shape=[jax.ShapeDtypeStruct((F,T),bf),jax.ShapeDtypeStruct((T,F),bf),jax.ShapeDtypeStruct((T,F),bf)],
        compiler_params=pltpu.CompilerParams(vmem_limit_bytes=VM),name="p2")(a,dy,wg,wu,wd)
import math
MESH=pl.DeviceIdType.MESH
div,rem=lax.div,lax.rem

def mega(n,hid1T,a1T,hid0T,a0T,dy,dg1,du1,wg,wu,wd,s0,t0,h1,mg,mu,md,vg,vu,vd,axis="dp"):
    T,Dm=dy.shape; L,_,F=wg.shape
    S=math.isqrt(n//2); R=Dm//n; Q=Dm//4; K=F//Dm
    assert S==4 and 2*S*S==n and F==4*Dm and L==2 and R%16==0 and Q%128==0
    U=3*L*K; N=U+8; TM=T//4
    hv=lambda h: h.reshape(S,S,2,K,R,T)
    av=lambda a: a.reshape(S,S,2,R,T)
    def kern(hid1T,a1T,hid0T,a0T,dy,dg1,du1,wg,wu,wd,s0,t0,h1,mg,mu,md,vg,vu,vd,
             wag,gsum,dg0,du0,
             lhs,rhs,own,dsend,drecv,r1,r2,r3,e1,e2,e3,pf,q1,q2,q3,x1,x2,x3,wst,win,min_,vin,gst,
             wbuf,gt,ut,ht,yt,st,tt,
             lsem,rsem,wsem,gsem,ssem,osem,isem,nsem,csem,
             dss,drs,ss,rs,ads,adr):
        me=lax.axis_index(axis)
        c=rem(me,2); y=rem(div(me,2),S); x=div(me,2*S)
        idx=lambda x,y,c: (rem(x+S,S)*S+rem(y+S,S))*2+c
        nb=[idx(x+1,y,c),idx(x-1,y,c),idx(x,y+1,c),idx(x,y-1,c)]; pa=idx(x,y,1-c)
        AB=[(x,y),(y,x)]
        P1=[(0,1),(2,3)]; P2=[(2,3),(0,1)]
        def rc(src,dst,s,r,dev):
            return pltpu.make_async_remote_copy(src_ref=src,dst_ref=dst,send_sem=s,recv_sem=r,device_id={axis:dev},device_id_type=MESH)
        cp=pltpu.make_async_copy
        def jk(u):
            l,v=div(u,3*K),rem(u,3*K); w=v-K
            return 3*l+jnp.where(v<K,0,1+rem(w,2)),jnp.where(v<K,v,div(w,2))
        def loc(u): j,k=jk(u); return j*K+k
        two=lambda u: rem(u,2)
        four=lambda u: rem(u,4)
        def sems(kind,u,d): return ss.at[kind,two(u),d],rs.at[kind,four(u),d],nb[d]
        m1,m2,m3,o1,o2,o3=(lambda u,d,kind=kind,e=e,r=r: rc(e.at[two(u),d],r.at[four(u),d],*sems(kind,u,d))
                           for kind,(e,r) in enumerate(((e1,r1),(e2,r2),(e3,r3),(x1,q1),(x2,q2),(x3,q3))))
        pair=lambda g: pl.ds(2*g,2)
        up_,down_=(lambda v: rem(v+1,S)),(lambda v: rem(v+S-1,S))
        behind=lambda v,s: (down_,up_)[s](v)
        far_=lambda v: rem(v+2,S)
        def g1(u,g,s):
            a,b=AB[g]; d=P2[g][s]
            return rc(wst.at[two(u),pair(g)],wag.at[loc(u),c,pair(g),a,b],*sems(6,u,d))
        def g2(u,g,s):
            a,b=AB[g]; d=P2[g][s]; r=wag.at[loc(u),c,2*g+s,a,behind(b,s)]
            return rc(r,r,*sems(7,u,d))
        def g3(u,g,s):
            a,b=AB[g]; d=P1[g][s]; r=wag.at[loc(u),c,pair(g),a]
            return rc(r,r,*sems(8,u,d))
        def g4(u,g,s):
            a,b=AB[g]; d=P1[g][s]; r=wag.at[loc(u),c,2*g+s,behind(a,s)]
            return rc(r,r,*sems(9,u,d))
        def d2(u): return rc(dsend,drecv.at[four(u)],dss,drs.at[four(u)],pa)
        def gd(u): return rc(wag.at[loc(u),c],wag.at[loc(u),c],ads.at[two(u)],adr.at[four(u)],pa)
        GS=[(g,s) for g in range(2) for s in range(2)]
        f=lambda v: v.astype(f32)
        def lhs_load(u,h):
            j,k=jk(u); cc=(1-c) if h else c; dst=lhs.at[h]; sem=lsem.at[h]
            @pl.when(j==0)
            def _(): cp(hid1T.at[:,:,cc,k],dst,sem).start()
            @pl.when(u==K)
            def _(): cp(a1T.at[:,:,cc],dst,sem).start()
            @pl.when(j==3)
            def _(): cp(hid0T.at[:,:,cc,k],dst,sem).start()
            @pl.when(u==4*K)
            def _(): cp(a0T.at[:,:,cc],dst,sem).start()
        def lhs_wait(u,h):
            @pl.when(rem(u,3*K)<=K)
            def _(): cp(a1T.at[:,:,c],lhs.at[h],lsem.at[h]).wait()
        def rhs_load(u):
            j,k=jk(u); dst=rhs.at[0]; sem=rsem; cols=pl.ds(pl.multiple_of(k*Dm,Dm),Dm)
            @pl.when(u==0)
            def _(): cp(dy,dst,sem).start()
            @pl.when(j==1)
            def _(): cp(dg1.at[:,cols],dst,sem).start()
            @pl.when(j==2)
            def _(): cp(du1.at[:,cols],dst,sem).start()
            @pl.when(j==4)
            def _(): cp(dg0.at[:,cols],dst,sem).start()
            @pl.when(j==5)
            def _(): cp(du0.at[:,cols],dst,sem).start()
        def rhs_wait(u):
            @pl.when((u==0)|(rem(u,3*K)>=K))
            def _(): cp(dy,rhs.at[0],rsem).wait()
        def state(u,go):
            j,k=jk(u); l=1-div(j,3); t=rem(j,3); sl=two(u)
            cols=pl.ds(pl.multiple_of(k*Dm,Dm),Dm)
            def three(mr,vr,wr):
                go(cp(mr,min_.at[sl],isem.at[0,sl])); go(cp(vr,vin.at[sl],isem.at[1,sl])); go(cp(wr,win.at[sl],isem.at[2,sl]))
            @pl.when(t==0)
            def _():
                r=pl.ds(pl.multiple_of(k*R,R),R)
                three(md.at[l,r],vd.at[l,r],wd.at[l,pl.ds(pl.multiple_of(me*(K*R)+k*R,R),R)])
            @pl.when(t==1)
            def _(): three(mg.at[l,:,cols],vg.at[l,:,cols],wg.at[l,pl.ds(pl.multiple_of(me*R,R),R),cols])
            @pl.when(t==2)
            def _(): three(mu.at[l,:,cols],vu.at[l,:,cols],wu.at[l,pl.ds(pl.multiple_of(me*R,R),R),cols])
        start=lambda d: d.start()
        wait=lambda d: d.wait()
        def both(q,o,u): return f(own[rem(u,3),q,o])+f(drecv[four(u),q,o])
        def at(i,dl,body):
            u=i-dl
            @pl.when((u>=0)&(u<U))
            def _(): body(u)
        def sA1(u):
            d2(u).wait()
            sl=four(u); w=two(u)
            for g in range(2):
                a,b=AB[g]; p,m=P1[g]
                far=far_(a)
                e1[w,p]=both(2*g,far,u).astype(bf); m1(u,p).start()
                e1[w,m]=both(2*g+1,far,u).astype(bf); m1(u,m).start()
            for g in range(2):
                a,b=AB[g]; p,m=P1[g]
                e2[w,p]=both(2*g+1,up_(a),u).astype(bf); m2(u,p).start()
                e2[w,m]=both(2*g,down_(a),u).astype(bf); m2(u,m).start()
        def sA2(u):
            sl=four(u); w=two(u)
            for d in range(4): m1(u,d).wait_send(); m2(u,d).wait_send()
            for g in range(2):
                a,b=AB[g]; p,m=P1[g]
                m1(u,p).wait_recv()
                e3[w,p]=(both(2*g,up_(a),u)+f(r1[sl,p])).astype(bf); m3(u,p).start()
                m1(u,m).wait_recv()
                e3[w,m]=(both(2*g+1,down_(a),u)+f(r1[sl,m])).astype(bf); m3(u,m).start()
        def sA3(u):
            sl=four(u); w=two(u)
            for d in range(4): m3(u,d).wait_send()
            for g in range(2):
                a,b=AB[g]; p,m=P1[g]
                for d in (p,m): m2(u,d).wait_recv(); m3(u,d).wait_recv()
                pf[w,2*g]=both(2*g,a,u)+f(r3[sl,p])+f(r2[sl,m])
                pf[w,2*g+1]=both(2*g+1,a,u)+f(r2[sl,p])+f(r3[sl,m])
                p,m=P2[g]; far=far_(b)
                x1[w,p]=pf[w,2*g,far].astype(bf); o1(u,p).start()
                x1[w,m]=pf[w,2*g+1,far].astype(bf); o1(u,m).start()
                x2[w,p]=pf[w,2*g+1,up_(b)].astype(bf); o2(u,p).start()
                x2[w,m]=pf[w,2*g,down_(b)].astype(bf); o2(u,m).start()
        def sB3(u):
            sl=four(u); w=two(u)
            for g in range(2):
                a,b=AB[g]; p,m=P2[g]
                o1(u,p).wait_recv()
                x3[w,p]=(pf[w,2*g,up_(b)]+f(q1[sl,p])).astype(bf); o3(u,p).start()
                o1(u,m).wait_recv()
                x3[w,m]=(pf[w,2*g+1,down_(b)]+f(q1[sl,m])).astype(bf); o3(u,m).start()
            for d in range(4): o1(u,d).wait_send(); o2(u,d).wait_send()
        def sA4(u):
            sl=four(u); w=two(u)
            state(u,wait)
            for d in range(4): o3(u,d).wait_send()
            for g in range(2):
                a,b=AB[g]; p,m=P2[g]
                for d in (p,m): o2(u,d).wait_recv(); o3(u,d).wait_recv()
                for h in range(2):
                    q=2*g+h
                    tot=pf[w,q,b]+(f(q3[sl,p])+f(q2[sl,m]) if h==0 else f(q2[sl,p])+f(q3[sl,m]))
                    gr=f(tot.astype(bf)); cs=slice(q*Q,(q+1)*Q)
                    mn=0.9*min_[w,:,cs]+0.1*gr
                    vn=0.95*vin[w,:,cs]+0.05*gr*gr
                    wo=f(win[w,:,cs])
                    wst[w,q]=(wo-0.02*(mn*lax.rsqrt(vn+1e-8)+0.1*wo)).astype(bf)
                    gst[w,:,cs]=gr.astype(bf)
                for s in range(2): g1(u,g,s).start()
                cp(wst.at[w,pair(g)],wag.at[loc(u),c,pair(g),a,b],csem.at[w,g]).start()
            cp(gst.at[w],gsum.at[loc(u)],nsem.at[w]).start()
        def sB4(u):
            for g,s in GS:
                g1(u,g,s).wait_recv(); g2(u,g,s).start()
        def sB5(u):
            w=rem(u,2)
            for g,s in GS:
                g1(u,g,s).wait_send(); g2(u,g,s).wait_send()
            for g in range(2):
                a,b=AB[g]
                cp(wst.at[w,pair(g)],wag.at[loc(u),c,pair(g),a,b],csem.at[w,g]).wait()
                for s in range(2): g2(u,g,s).wait_recv()
                for s in range(2): g3(u,g,s).start()
            cp(gst.at[w],gsum.at[loc(u)],nsem.at[w]).wait()
        def sB6(u):
            for g,s in GS: g3(u,g,s).wait_send()
            for g,s in GS:
                g3(u,g,s).wait_recv(); g4(u,g,s).start()
        def sB7(u):
            for g,s in GS: g4(u,g,s).wait()
            gd(u).start()
        def sB8(u): gd(u).wait()
        def part(u,h):
            lhs_wait(u,h)
            rsl=jnp.where(jk(u)[0]==3,1,0)
            for q in range(4):
                o=dot(lhs[h].reshape(S*S*R,T),rhs[rsl,:,q*Q:(q+1)*Q]).astype(bf)
                for A in range(S):
                    for B in range(S):
                        blk=o[(A*S+B)*R:(A*S+B+1)*R]
                        o_,i_=(A,B) if q<2 else (B,A)
                        if h: dsend[q,o_,i_]=blk
                        else: own[rem(u,3),q,o_,i_]=blk
            @pl.when(u+1<U)
            def _(): lhs_load(u+1,h)
        tiles=lambda r: pl.ds(pl.multiple_of(r*TM,TM),TM)
        def da_load(v):
            r,h=div(v,2),rem(v,2); rr=tiles(r)
            @pl.when(h==0)
            def _(): cp(du1.at[rr],gt,gsem.at[0]).start()
            @pl.when(h==1)
            def _():
                cp(dg1.at[rr],gt,gsem.at[0]).start()
                cp(h1.at[rr],ht,gsem.at[1]).start(); cp(dy.at[rr],yt,gsem.at[2]).start()
        def w1_load(): return [cp(wu.at[1],wbuf.at[0],wsem.at[0]),cp(wg.at[1],wbuf.at[1],wsem.at[1])]
        def wd_load(): return [cp(wd.at[0,pl.ds(k*Dm,Dm)],wbuf.at[0,:,pl.ds(k*Dm,Dm)],wsem.at[2+k]) for k in range(K)]
        def da_slice(v):
            r,h=div(v,2),rem(v,2); rr=tiles(r)
            @pl.when(v==0)
            def _():
                for d in w1_load(): d.wait()
            cp(du1.at[rr],gt,gsem.at[0]).wait()
            da=dot_nt(gt[...],wbuf[h]).astype(bf)
            @pl.when(h==0)
            def _(): ut[...]=da
            @pl.when(h==1)
            def _():
                cp(h1.at[rr],ht,gsem.at[1]).wait(); cp(dy.at[rr],yt,gsem.at[2]).wait()
                db=f((f(da)+f(ut[...])).astype(bf))
                wide=f(ht[...])
                sc=lax.rsqrt(jnp.mean(wide*wide,-1,keepdims=True)+1e-6)
                dn=db*sc-wide*(sc*sc*sc*jnp.mean(db*wide,-1,keepdims=True))
                rhs[1,rr,:]=(f(yt[...])+f(dn.astype(bf))).astype(bf)
            @pl.when(v<7)
            def _(): da_load(v+1)
            @pl.when(v==7)
            def _():
                for d in wd_load(): d.start()
                for r in (0,1):
                    for d in st_load(0,r): d.start()
        HC=Dm//2
        def st_load(v,r):
            cc=pl.ds(pl.multiple_of(v*HC,HC),HC); rr=pl.ds(r*TM,TM); sl=r%2
            return [cp(s0.at[rr,cc],st.at[sl],ssem.at[0,sl]),cp(t0.at[rr,cc],tt.at[sl],ssem.at[1,sl])]
        def put(v,r):
            cc=pl.ds(pl.multiple_of(v*HC,HC),HC); rr=pl.ds(r*TM,TM)
            return [cp(gt.at[:,pl.ds((2*r+h)*HC,HC)],o.at[rr,cc],osem.at[h,r]) for h,o in enumerate((dg0,du0))]
        def dh_slice(v,rs):
            k=div(v,2); w=wbuf[0,pl.ds(pl.multiple_of(rem(v,2)*HC,HC),HC),pl.ds(pl.multiple_of(k*Dm,Dm),Dm)]
            for r in rs:
                for d in st_load(v,r): d.wait()
                dh=f(dot_nt(rhs[1,r*TM:(r+1)*TM,:],w).astype(bf))
                gt[:,(2*r)*HC:(2*r+1)*HC]=(dh*tt[r%2]).astype(bf)
                gt[:,(2*r+1)*HC:(2*r+2)*HC]=(dh*st[r%2]).astype(bf)
                for d in put(v,r): d.start()
        def dh_first(v):
            @pl.when(v==0)
            def _():
                for d in wd_load(): d.wait()
            @pl.when(v>0)
            def _():
                for r in (2,3):
                    for d in put(v-1,r): d.wait()
            dh_slice(v,(0,1))
            for r in (2,3):
                for d in st_load(v,r): d.start()
        def dh_second(v):
            dh_slice(v,(2,3))
            for r in (0,1):
                for d in put(v,r): d.wait()
            @pl.when(v<2*K-1)
            def _():
                for r in (0,1):
                    for d in st_load(v+1,r): d.start()
            @pl.when(v==2*K-1)
            def _():
                for r in (2,3):
                    for d in put(v,r): d.wait()
        lhs_load(0,1); rhs_load(0); lhs_load(0,0)
        bar=pltpu.get_barrier_semaphore()
        for d in nb+[pa]:
            pl.semaphore_signal(bar,inc=1,device_id={axis:d},device_id_type=MESH)
        pl.semaphore_wait(bar,5)
        da_load(0)
        for d in w1_load(): d.start()
        @pl.loop(0,N)
        def _(i):
            at(i,4,sA4); at(i,3,sA3); at(i,2,sA2); at(i,1,sA1)
            @pl.when(i<U)
            def _():
                rhs_wait(i)
                part(i,1)
                d2(i).start()
            at(i,3,sB3); at(i,4,sB4); at(i,5,sB5); at(i,6,sB6); at(i,7,sB7); at(i,8,sB8)
            at(i,3,lambda u: state(u,start))
            @pl.when((i>=12)&(i<12+2*K))
            def _(): dh_first(i-12)
            @pl.when(i<U)
            def _():
                part(i,0)
                @pl.when(i+1<U)
                def _(): rhs_load(i+1)
            @pl.when((i>=4)&(i<12))
            def _(): da_slice(i-4)
            @pl.when((i>=12)&(i<12+2*K))
            def _(): dh_second(i-12)
    A=pl.BlockSpec(memory_space=pl.ANY)
    sd=jax.ShapeDtypeStruct
    V=pltpu.VMEM; DS=pltpu.SemaphoreType.DMA
    msg=lambda k: V((k,4,S,R,Q),bf)
    small=lambda k: V((k,4,R,Q),bf)
    out=pl.pallas_call(kern,
        in_specs=[A]*19,out_specs=[A]*4,
        out_shape=[sd((U,2,4,S,S,R,Q),bf)]+[sd((U,R,Dm),bf)]+[sd((T,F),bf)]*2,
        scratch_shapes=[V((2,S,S,R,T),bf),V((2,T,Dm),bf),V((3,4,S,S,R,Q),bf),V((4,S,S,R,Q),bf),V((4,4,S,S,R,Q),bf),
            msg(4),msg(4),msg(4),msg(2),msg(2),msg(2),V((2,4,S,R,Q),f32),
            small(4),small(4),small(4),small(2),small(2),small(2),
            V((2,4,R,Q),bf),V((2,R,Dm),bf),V((2,R,Dm),f32),V((2,R,Dm),f32),V((2,R,Dm),bf),
            V((2,Dm,F),bf),V((TM,F),bf),V((TM,Dm),bf),V((TM,Dm),bf),V((TM,Dm),bf),V((2,TM,Dm//2),f32),V((2,TM,Dm//2),f32),
            DS((2,)),DS(()),DS((2+K,)),DS((3,)),DS((2,2)),DS((2,4)),DS((3,2)),DS((2,)),DS((2,2)),
            DS(()),DS((4,)),DS((10,2,4)),DS((10,4,4)),DS((2,)),DS((4,))],
        compiler_params=pltpu.CompilerParams(collective_id=0,has_side_effects=True,vmem_limit_bytes=67043328),name="mega",
    )(hv(hid1T),av(a1T),hv(hid0T),av(a0T),dy,dg1,du1,wg,wu,wd,s0,t0,h1,mg,mu,md,vg,vu,vd)
    return out

def final(wag,gsum,ms,vs):
    U,_,_,S,_,R,Q=wag.shape; n=2*S*S; Dm=4*Q; L=ms[0].shape[0]; K=U//(3*L)
    ms=(ms[0].reshape(L,K,R,Dm),*ms[1:]); vs=(vs[0].reshape(L,K,R,Dm),*vs[1:])
    B=2
    def kern(w_ref,g_ref,*refs):
        m,v,wo,mo,vo=(refs[3*i:3*i+3] for i in range(5))
        kind=div(B*pl.program_id(0),L*K)
        for t in range(3):
            @pl.when(kind==t)
            def _():
                for p in range(B):
                    for cc in range(2):
                        for r in range(S*S):
                            for q in range(4):
                                v_=w_ref[p,cc,q,r//S,r%S] if q<2 else w_ref[p,cc,q,r%S,r//S]
                                if t: wo[t][0,(2*r+cc)*R:(2*r+cc+1)*R,p*Dm+q*Q:p*Dm+q*Q+Q]=v_
                                else: wo[t][0,2*r+cc,p,:,q*Q:q*Q+Q]=v_
                    g=g_ref[p].astype(f32)
                    at=(0,slice(None),slice(p*Dm,p*Dm+Dm)) if t else (0,p)
                    mo[t][at]=0.9*m[t][at]+0.1*g
                    vo[t][at]=0.95*v[t][at]+0.05*g*g
    H=K//B; E=L*H
    def lk(s,t): s=jnp.clip(s-t*E,0,E-1); return div(s,H),rem(s,H)
    def unit(s): l,k=lk(rem(s,E),0); return ((L-1-l)*3+div(s,E))*H+k
    def spec(t,d,g):
        def at(s): l,k=lk(s,t); return (l,0,k) if t else (l,*[0]*(len(d)-4),k,0,0)
        return pl.BlockSpec(g if t else d,at)
    sd=jax.ShapeDtypeStruct
    mom=[spec(t,(1,B,R,Dm),(1,R,B*Dm)) for t in range(3)]
    o=pl.pallas_call(kern,grid=(U//B,),
        in_specs=[pl.BlockSpec((B,2,4,S,S,R,Q),lambda s:(unit(s),*[0]*6)),pl.BlockSpec((B,R,Dm),lambda s:(unit(s),0,0))]+mom*2,
        out_specs=[spec(t,(1,n,B,R,Dm),(1,Dm,B*Dm)) for t in range(3)]+mom*2,
        out_shape=[sd((L,n,K,R,Dm),bf),sd((L,Dm,K*Dm),bf),sd((L,Dm,K*Dm),bf)]+[sd(a.shape,f32) for a in (*ms,*vs)],
        name="final",compiler_params=pltpu.CompilerParams(vmem_limit_bytes=VM))(wag,gsum,*ms,*vs)
    w,m,v=o[:3],o[3:6],o[6:]
    order=lambda d,g,u: (g,u,d.reshape(L,-1,Dm))
    return (*order(*w),*order(*m),*order(*v))

def solution(mesh):
    from jax.sharding import PartitionSpec as P
    n=mesh.shape["dp"]
    def step(x,dy,wg,wu,wd,mg,mu,md,vg,vu,vd):
        x,dy=x[0],dy[0]
        hid0T,s0,t0,a0T,h1,a1,a1T=p01(x,wg,wu,wd)
        hid1T,dg1,du1=p2(a1,dy,wg,wu,wd,1)
        wag,gsum,_,_=mega(n,hid1T,a1T,hid0T,a0T,dy,dg1,du1,wg,wu,wd,s0,t0,h1,mg,mu,md,vg,vu,vd)
        return final(wag,gsum,(md,mg,mu),(vd,vg,vu))
    tok=P(("rep","dp"),None,None); w=P(None,None,None); m=P(None,"dp",None)
    return jax.shard_map(step,mesh=mesh,in_specs=(tok,tok,w,w,w)+(m,)*6,
        out_specs=(P("rep",None,None),)*3+(P("rep","dp",None),)*6,check_vma=False)
```

```python
import functools
import jax, jax.numpy as jnp
from jax import lax
from jax.experimental import pallas as pl
from jax.experimental.pallas import tpu as pltpu
bf=jnp.bfloat16; f32=jnp.float32
VM=62*2**20
def dot(a,b): return jnp.dot(a,b,preferred_element_type=f32)
def dot_nt(a,b): return lax.dot_general(a,b,(((1,),(1,)),((),())),preferred_element_type=f32)
def normed(h):
    wide=h.astype(f32)
    return (wide*lax.rsqrt(jnp.mean(wide**2,-1,keepdims=True)+1e-6)).astype(bf)

def p01(x,wg,wu,wd,tm=512,tf=1024,rm=256,rf=256):
    T,Dm=x.shape; F=wg.shape[-1]; nf=F//tf
    def kern(x_ref,wg,wu,wd,hidT_ref,s_ref,t_ref,aT_ref,h_ref,a_ref,a1T_ref,gs,us,ds,a_sc,hid_sc,acc,sem):
        t,f=pl.program_id(0),pl.program_id(1)
        part=lambda f: pl.ds(pl.multiple_of(f*tf,tf),tf)
        def loads(f):
            p=part(f)
            return [pltpu.make_async_copy(a,b,sem.at[i,f]) for i,(a,b) in enumerate(((wg.at[0,:,p],gs.at[:,p]),(wu.at[0,:,p],us.at[:,p]),(wd.at[0,p],ds.at[p])))]
        @pl.when((t==0)&(f==0))
        def _():
            for g in range(nf):
                for d in loads(g): d.start()
        @pl.when(f==0)
        def _():
            a=normed(x_ref[...])
            a_sc[...]=a
            aT_ref[...]=a.T
            acc[...]=jnp.zeros_like(acc)
        @pl.when(t==0)
        def _():
            for d in loads(f): d.wait()
        for r in range(tm//rm):
            rs=slice(r*rm,(r+1)*rm); a=a_sc[rs,:]
            for c in range(tf//rf):
                cs=slice(c*rf,(c+1)*rf); cols=pl.ds(pl.multiple_of(f*tf+c*rf,rf),rf)
                gate=dot(a,gs[:,cols]); up=dot(a,us[:,cols])
                sg=jax.nn.sigmoid(gate); s=gate*sg
                s_ref[rs,cs]=s
                t_ref[rs,cs]=up*(sg*(1.0+gate*(1.0-sg)))
                hid=(s*up).astype(bf)
                hid_sc[rs,cs]=hid
                hidT_ref[cs,rs]=hid.T
        acc[...]+=dot(hid_sc[...],ds[part(f),:])
        @pl.when(f==nf-1)
        def _():
            h=x_ref[...]+acc[...].astype(bf)
            h_ref[...]=h
            a=normed(h)
            a_ref[...]=a
            a1T_ref[...]=a.T
    A=pl.BlockSpec(memory_space=pl.ANY)
    row=pl.BlockSpec((tm,Dm),lambda t,f:(t,0)); col=pl.BlockSpec((Dm,tm),lambda t,f:(0,t)); tile=pl.BlockSpec((tm,tf),lambda t,f:(t,f))
    sd=jax.ShapeDtypeStruct; V=pltpu.VMEM
    return pl.pallas_call(kern,grid=(T//tm,nf),in_specs=[row,A,A,A],
        out_specs=[pl.BlockSpec((tf,tm),lambda t,f:(f,t)),tile,tile,col,row,row,col],
        out_shape=[sd((F,T),bf),sd((T,F),f32),sd((T,F),f32),sd((Dm,T),bf),sd((T,Dm),bf),sd((T,Dm),bf),sd((Dm,T),bf)],
        scratch_shapes=[V((Dm,F),bf),V((Dm,F),bf),V((F,Dm),bf),V((tm,Dm),bf),V((tm,tf),bf),V((tm,Dm),f32),pltpu.SemaphoreType.DMA((3,nf))],
        compiler_params=pltpu.CompilerParams(vmem_limit_bytes=VM),name="p01")(x,wg,wu,wd)

def p2(a,dy,wg,wu,wd,layer,tm=1024,tf=512,rm=256,rf=256):
    T,Dm=a.shape; F=wg.shape[-1]
    def kern(a_ref,dy_ref,wg_ref,wu_ref,wd_ref,hidT_ref,dg_ref,du_ref):
        t=pl.program_id(1)
        for r in range(tm//rm):
            ro=slice(r*rm,(r+1)*rm)
            av=a_ref[ro,:]; dv=dy_ref[ro,:]
            for c in range(tf//rf):
                cs=slice(c*rf,(c+1)*rf); rs=slice(r*rm,(r+1)*rm)
                gate=dot(av,wg_ref[0,:,cs]); up=dot(av,wu_ref[0,:,cs])
                dh=dot_nt(dv,wd_ref[0,cs,:]).astype(bf).astype(f32)
                sg=jax.nn.sigmoid(gate); s=gate*sg
                du_ref[rs,cs]=(dh*s).astype(bf)
                dg_ref[rs,cs]=(dh*(up*(sg*(1.0+gate*(1.0-sg))))).astype(bf)
                hidT_ref[cs,rs]=(s*up).astype(bf).T
    return pl.pallas_call(kern,grid=(F//tf,T//tm),
        in_specs=[pl.BlockSpec((tm,Dm),lambda f,t:(t,0)),pl.BlockSpec((tm,Dm),lambda f,t:(t,0)),
                  pl.BlockSpec((1,Dm,tf),lambda f,t:(layer,0,f)),pl.BlockSpec((1,Dm,tf),lambda f,t:(layer,0,f)),pl.BlockSpec((1,tf,Dm),lambda f,t:(layer,f,0))],
        out_specs=[pl.BlockSpec((tf,tm),lambda f,t:(f,t)),pl.BlockSpec((tm,tf),lambda f,t:(t,f)),pl.BlockSpec((tm,tf),lambda f,t:(t,f))],
        out_shape=[jax.ShapeDtypeStruct((F,T),bf),jax.ShapeDtypeStruct((T,F),bf),jax.ShapeDtypeStruct((T,F),bf)],
        compiler_params=pltpu.CompilerParams(vmem_limit_bytes=VM),name="p2")(a,dy,wg,wu,wd)
import math
MESH=pl.DeviceIdType.MESH
div,rem=lax.div,lax.rem

def mega(n,hid1T,a1T,hid0T,a0T,dy,dg1,du1,wg,wu,wd,s0,t0,h1,mg,mu,md,vg,vu,vd,axis="dp"):
    T,Dm=dy.shape; L,_,F=wg.shape
    S=math.isqrt(n//2); R=Dm//n; Q=Dm//4; K=F//Dm
    assert S==4 and 2*S*S==n and F==4*Dm and L==2 and R%16==0 and Q%128==0
    U=3*L*K; N=U+8; TM=T//4
    hv=lambda h: h.reshape(S,S,2,K,R,T)
    av=lambda a: a.reshape(S,S,2,R,T)
    def kern(hid1T,a1T,hid0T,a0T,dy,dg1,du1,wg,wu,wd,s0,t0,h1,mg,mu,md,vg,vu,vd,
             wag,gsum,dg0,du0,
             lhs,rhs,own,dsend,drecv,r1,r2,r3,e1,e2,e3,pf,q1,q2,q3,x1,x2,x3,wst,win,min_,vin,gst,
             wbuf,gt,ut,ht,yt,st,tt,
             lsem,rsem,wsem,gsem,ssem,osem,isem,nsem,csem,
             dss,drs,ss,rs,ads,adr):
        me=lax.axis_index(axis)
        c=rem(me,2); y=rem(div(me,2),S); x=div(me,2*S)
        idx=lambda x,y,c: (rem(x+S,S)*S+rem(y+S,S))*2+c
        nb=[idx(x+1,y,c),idx(x-1,y,c),idx(x,y+1,c),idx(x,y-1,c)]; pa=idx(x,y,1-c)
        AB=[(x,y),(y,x)]
        P1=[(0,1),(2,3)]; P2=[(2,3),(0,1)]
        def rc(src,dst,s,r,dev):
            return pltpu.make_async_remote_copy(src_ref=src,dst_ref=dst,send_sem=s,recv_sem=r,device_id={axis:dev},device_id_type=MESH)
        cp=pltpu.make_async_copy
        def jk(u):
            l,v=div(u,3*K),rem(u,3*K); w=v-K
            return 3*l+jnp.where(v<K,0,1+rem(w,2)),jnp.where(v<K,v,div(w,2))
        def loc(u): j,k=jk(u); return j*K+k
        two=lambda u: rem(u,2)
        four=lambda u: rem(u,4)
        def sems(kind,u,d): return ss.at[kind,two(u),d],rs.at[kind,four(u),d],nb[d]
        m1,m2,m3,o1,o2,o3=(lambda u,d,kind=kind,e=e,r=r: rc(e.at[two(u),d],r.at[four(u),d],*sems(kind,u,d))
                           for kind,(e,r) in enumerate(((e1,r1),(e2,r2),(e3,r3),(x1,q1),(x2,q2),(x3,q3))))
        pair=lambda g: pl.ds(2*g,2)
        up_,down_=(lambda v: rem(v+1,S)),(lambda v: rem(v+S-1,S))
        behind=lambda v,s: (down_,up_)[s](v)
        far_=lambda v: rem(v+2,S)
        def g1(u,g,s):
            a,b=AB[g]; d=P2[g][s]
            return rc(wst.at[two(u),pair(g)],wag.at[loc(u),c,pair(g),a,b],*sems(6,u,d))
        def g2(u,g,s):
            a,b=AB[g]; d=P2[g][s]; r=wag.at[loc(u),c,2*g+s,a,behind(b,s)]
            return rc(r,r,*sems(7,u,d))
        def g3(u,g,s):
            a,b=AB[g]; d=P1[g][s]; r=wag.at[loc(u),c,pair(g),a]
            return rc(r,r,*sems(8,u,d))
        def g4(u,g,s):
            a,b=AB[g]; d=P1[g][s]; r=wag.at[loc(u),c,2*g+s,behind(a,s)]
            return rc(r,r,*sems(9,u,d))
        def d2(u): return rc(dsend,drecv.at[four(u)],dss,drs.at[four(u)],pa)
        def gd(u): return rc(wag.at[loc(u),c],wag.at[loc(u),c],ads.at[two(u)],adr.at[four(u)],pa)
        GS=[(g,s) for g in range(2) for s in range(2)]
        f=lambda v: v.astype(f32)
        def lhs_load(u,h):
            j,k=jk(u); cc=(1-c) if h else c; dst=lhs.at[h]; sem=lsem.at[h]
            @pl.when(j==0)
            def _(): cp(hid1T.at[:,:,cc,k],dst,sem).start()
            @pl.when(u==K)
            def _(): cp(a1T.at[:,:,cc],dst,sem).start()
            @pl.when(j==3)
            def _(): cp(hid0T.at[:,:,cc,k],dst,sem).start()
            @pl.when(u==4*K)
            def _(): cp(a0T.at[:,:,cc],dst,sem).start()
        def lhs_wait(u,h):
            @pl.when(rem(u,3*K)<=K)
            def _(): cp(a1T.at[:,:,c],lhs.at[h],lsem.at[h]).wait()
        def rhs_load(u):
            j,k=jk(u); dst=rhs.at[0]; sem=rsem; cols=pl.ds(pl.multiple_of(k*Dm,Dm),Dm)
            @pl.when(u==0)
            def _(): cp(dy,dst,sem).start()
            @pl.when(j==1)
            def _(): cp(dg1.at[:,cols],dst,sem).start()
            @pl.when(j==2)
            def _(): cp(du1.at[:,cols],dst,sem).start()
            @pl.when(j==4)
            def _(): cp(dg0.at[:,cols],dst,sem).start()
            @pl.when(j==5)
            def _(): cp(du0.at[:,cols],dst,sem).start()
        def rhs_wait(u):
            @pl.when((u==0)|(rem(u,3*K)>=K))
            def _(): cp(dy,rhs.at[0],rsem).wait()
        def state(u,go):
            j,k=jk(u); l=1-div(j,3); t=rem(j,3); sl=two(u)
            cols=pl.ds(pl.multiple_of(k*Dm,Dm),Dm)
            def three(mr,vr,wr):
                go(cp(mr,min_.at[sl],isem.at[0,sl])); go(cp(vr,vin.at[sl],isem.at[1,sl])); go(cp(wr,win.at[sl],isem.at[2,sl]))
            @pl.when(t==0)
            def _():
                r=pl.ds(pl.multiple_of(k*R,R),R)
                three(md.at[l,r],vd.at[l,r],wd.at[l,pl.ds(pl.multiple_of(me*(K*R)+k*R,R),R)])
            @pl.when(t==1)
            def _(): three(mg.at[l,:,cols],vg.at[l,:,cols],wg.at[l,pl.ds(pl.multiple_of(me*R,R),R),cols])
            @pl.when(t==2)
            def _(): three(mu.at[l,:,cols],vu.at[l,:,cols],wu.at[l,pl.ds(pl.multiple_of(me*R,R),R),cols])
        start=lambda d: d.start()
        wait=lambda d: d.wait()
        def both(q,o,u): return f(own[rem(u,3),q,o])+f(drecv[four(u),q,o])
        def at(i,dl,body):
            u=i-dl
            @pl.when((u>=0)&(u<U))
            def _(): body(u)
        def sA1(u):
            d2(u).wait()
            sl=four(u); w=two(u)
            for g in range(2):
                a,b=AB[g]; p,m=P1[g]
                far=far_(a)
                e1[w,p]=both(2*g,far,u).astype(bf); m1(u,p).start()
                e1[w,m]=both(2*g+1,far,u).astype(bf); m1(u,m).start()
            for g in range(2):
                a,b=AB[g]; p,m=P1[g]
                e2[w,p]=both(2*g+1,up_(a),u).astype(bf); m2(u,p).start()
                e2[w,m]=both(2*g,down_(a),u).astype(bf); m2(u,m).start()
        def sA2(u):
            sl=four(u); w=two(u)
            for d in range(4): m1(u,d).wait_send(); m2(u,d).wait_send()
            for g in range(2):
                a,b=AB[g]; p,m=P1[g]
                m1(u,p).wait_recv()
                e3[w,p]=(both(2*g,up_(a),u)+f(r1[sl,p])).astype(bf); m3(u,p).start()
                m1(u,m).wait_recv()
                e3[w,m]=(both(2*g+1,down_(a),u)+f(r1[sl,m])).astype(bf); m3(u,m).start()
        def sA3(u):
            sl=four(u); w=two(u)
            for d in range(4): m3(u,d).wait_send()
            for g in range(2):
                a,b=AB[g]; p,m=P1[g]
                for d in (p,m): m2(u,d).wait_recv(); m3(u,d).wait_recv()
                pf[w,2*g]=both(2*g,a,u)+f(r3[sl,p])+f(r2[sl,m])
                pf[w,2*g+1]=both(2*g+1,a,u)+f(r2[sl,p])+f(r3[sl,m])
                p,m=P2[g]; far=far_(b)
                x1[w,p]=pf[w,2*g,far].astype(bf); o1(u,p).start()
                x1[w,m]=pf[w,2*g+1,far].astype(bf); o1(u,m).start()
                x2[w,p]=pf[w,2*g+1,up_(b)].astype(bf); o2(u,p).start()
                x2[w,m]=pf[w,2*g,down_(b)].astype(bf); o2(u,m).start()
        def sB3(u):
            sl=four(u); w=two(u)
            for g in range(2):
                a,b=AB[g]; p,m=P2[g]
                o1(u,p).wait_recv()
                x3[w,p]=(pf[w,2*g,up_(b)]+f(q1[sl,p])).astype(bf); o3(u,p).start()
                o1(u,m).wait_recv()
                x3[w,m]=(pf[w,2*g+1,down_(b)]+f(q1[sl,m])).astype(bf); o3(u,m).start()
            for d in range(4): o1(u,d).wait_send(); o2(u,d).wait_send()
        def sA4(u):
            sl=four(u); w=two(u)
            state(u,wait)
            for d in range(4): o3(u,d).wait_send()
            for g in range(2):
                a,b=AB[g]; p,m=P2[g]
                for d in (p,m): o2(u,d).wait_recv(); o3(u,d).wait_recv()
                for h in range(2):
                    q=2*g+h
                    tot=pf[w,q,b]+(f(q3[sl,p])+f(q2[sl,m]) if h==0 else f(q2[sl,p])+f(q3[sl,m]))
                    gr=f(tot.astype(bf)); cs=slice(q*Q,(q+1)*Q)
                    mn=0.9*min_[w,:,cs]+0.1*gr
                    vn=0.95*vin[w,:,cs]+0.05*gr*gr
                    wo=f(win[w,:,cs])
                    wst[w,q]=(wo-0.02*(mn*lax.rsqrt(vn+1e-8)+0.1*wo)).astype(bf)
                    gst[w,:,cs]=gr.astype(bf)
                for s in range(2): g1(u,g,s).start()
                cp(wst.at[w,pair(g)],wag.at[loc(u),c,pair(g),a,b],csem.at[w,g]).start()
            cp(gst.at[w],gsum.at[loc(u)],nsem.at[w]).start()
        def sB4(u):
            for g,s in GS:
                g1(u,g,s).wait_recv(); g2(u,g,s).start()
        def sB5(u):
            w=rem(u,2)
            for g,s in GS:
                g1(u,g,s).wait_send(); g2(u,g,s).wait_send()
            for g in range(2):
                a,b=AB[g]
                cp(wst.at[w,pair(g)],wag.at[loc(u),c,pair(g),a,b],csem.at[w,g]).wait()
                for s in range(2): g2(u,g,s).wait_recv()
                for s in range(2): g3(u,g,s).start()
            cp(gst.at[w],gsum.at[loc(u)],nsem.at[w]).wait()
        def sB6(u):
            for g,s in GS: g3(u,g,s).wait_send()
            for g,s in GS:
                g3(u,g,s).wait_recv(); g4(u,g,s).start()
        def sB7(u):
            for g,s in GS: g4(u,g,s).wait()
            gd(u).start()
        def sB8(u): gd(u).wait()
        def part(u,h):
            lhs_wait(u,h)
            rsl=jnp.where(jk(u)[0]==3,1,0)
            for q in range(4):
                o=dot(lhs[h].reshape(S*S*R,T),rhs[rsl,:,q*Q:(q+1)*Q]).astype(bf)
                for A in range(S):
                    for B in range(S):
                        blk=o[(A*S+B)*R:(A*S+B+1)*R]
                        o_,i_=(A,B) if q<2 else (B,A)
                        if h: dsend[q,o_,i_]=blk
                        else: own[rem(u,3),q,o_,i_]=blk
            @pl.when(u+1<U)
            def _(): lhs_load(u+1,h)
        tiles=lambda r: pl.ds(pl.multiple_of(r*TM,TM),TM)
        def da_load(v):
            r,h=div(v,2),rem(v,2); rr=tiles(r)
            @pl.when(h==0)
            def _(): cp(du1.at[rr],gt,gsem.at[0]).start()
            @pl.when(h==1)
            def _():
                cp(dg1.at[rr],gt,gsem.at[0]).start()
                cp(h1.at[rr],ht,gsem.at[1]).start(); cp(dy.at[rr],yt,gsem.at[2]).start()
        def w1_load(): return [cp(wu.at[1],wbuf.at[0],wsem.at[0]),cp(wg.at[1],wbuf.at[1],wsem.at[1])]
        def wd_load(): return [cp(wd.at[0,pl.ds(k*Dm,Dm)],wbuf.at[0,:,pl.ds(k*Dm,Dm)],wsem.at[2+k]) for k in range(K)]
        def da_slice(v):
            r,h=div(v,2),rem(v,2); rr=tiles(r)
            @pl.when(v==0)
            def _():
                for d in w1_load(): d.wait()
            cp(du1.at[rr],gt,gsem.at[0]).wait()
            da=dot_nt(gt[...],wbuf[h]).astype(bf)
            @pl.when(h==0)
            def _(): ut[...]=da
            @pl.when(h==1)
            def _():
                cp(h1.at[rr],ht,gsem.at[1]).wait(); cp(dy.at[rr],yt,gsem.at[2]).wait()
                db=f((f(da)+f(ut[...])).astype(bf))
                wide=f(ht[...])
                sc=lax.rsqrt(jnp.mean(wide*wide,-1,keepdims=True)+1e-6)
                dn=db*sc-wide*(sc*sc*sc*jnp.mean(db*wide,-1,keepdims=True))
                rhs[1,rr,:]=(f(yt[...])+f(dn.astype(bf))).astype(bf)
            @pl.when(v<7)
            def _(): da_load(v+1)
            @pl.when(v==7)
            def _():
                for d in wd_load(): d.start()
                for r in (0,1):
                    for d in st_load(0,r): d.start()
        HC=Dm//2
        def st_load(v,r):
            cc=pl.ds(pl.multiple_of(v*HC,HC),HC); rr=pl.ds(r*TM,TM); sl=r%2
            return [cp(s0.at[rr,cc],st.at[sl],ssem.at[0,sl]),cp(t0.at[rr,cc],tt.at[sl],ssem.at[1,sl])]
        def put(v,r):
            cc=pl.ds(pl.multiple_of(v*HC,HC),HC); rr=pl.ds(r*TM,TM)
            return [cp(gt.at[:,pl.ds((2*r+h)*HC,HC)],o.at[rr,cc],osem.at[h,r]) for h,o in enumerate((dg0,du0))]
        def dh_slice(v,rs):
            k=div(v,2); w=wbuf[0,pl.ds(pl.multiple_of(rem(v,2)*HC,HC),HC),pl.ds(pl.multiple_of(k*Dm,Dm),Dm)]
            for r in rs:
                for d in st_load(v,r): d.wait()
                dh=f(dot_nt(rhs[1,r*TM:(r+1)*TM,:],w).astype(bf))
                gt[:,(2*r)*HC:(2*r+1)*HC]=(dh*tt[r%2]).astype(bf)
                gt[:,(2*r+1)*HC:(2*r+2)*HC]=(dh*st[r%2]).astype(bf)
                for d in put(v,r): d.start()
        def dh_first(v):
            @pl.when(v==0)
            def _():
                for d in wd_load(): d.wait()
            @pl.when(v>0)
            def _():
                for r in (2,3):
                    for d in put(v-1,r): d.wait()
            dh_slice(v,(0,1))
            for r in (2,3):
                for d in st_load(v,r): d.start()
        def dh_second(v):
            dh_slice(v,(2,3))
            for r in (0,1):
                for d in put(v,r): d.wait()
            @pl.when(v<2*K-1)
            def _():
                for r in (0,1):
                    for d in st_load(v+1,r): d.start()
            @pl.when(v==2*K-1)
            def _():
                for r in (2,3):
                    for d in put(v,r): d.wait()
        lhs_load(0,1); rhs_load(0); lhs_load(0,0)
        bar=pltpu.get_barrier_semaphore()
        for d in nb+[pa]:
            pl.semaphore_signal(bar,inc=1,device_id={axis:d},device_id_type=MESH)
        pl.semaphore_wait(bar,5)
        da_load(0)
        for d in w1_load(): d.start()
        @pl.loop(0,N)
        def _(i):
            at(i,4,sA4); at(i,3,sA3); at(i,2,sA2); at(i,1,sA1)
            @pl.when(i<U)
            def _():
                rhs_wait(i)
                part(i,1)
                d2(i).start()
            at(i,3,sB3); at(i,4,sB4); at(i,5,sB5); at(i,6,sB6); at(i,7,sB7); at(i,8,sB8)
            at(i,3,lambda u: state(u,start))
            @pl.when((i>=12)&(i<12+2*K))
            def _(): dh_first(i-12)
            @pl.when(i<U)
            def _():
                part(i,0)
                @pl.when(i+1<U)
                def _(): rhs_load(i+1)
            @pl.when((i>=4)&(i<12))
            def _(): da_slice(i-4)
            @pl.when((i>=12)&(i<12+2*K))
            def _(): dh_second(i-12)
    A=pl.BlockSpec(memory_space=pl.ANY)
    sd=jax.ShapeDtypeStruct
    V=pltpu.VMEM; DS=pltpu.SemaphoreType.DMA
    msg=lambda k: V((k,4,S,R,Q),bf)
    small=lambda k: V((k,4,R,Q),bf)
    out=pl.pallas_call(kern,
        in_specs=[A]*19,out_specs=[A]*4,
        out_shape=[sd((U,2,4,S,S,R,Q),bf)]+[sd((U,R,Dm),bf)]+[sd((T,F),bf)]*2,
        scratch_shapes=[V((2,S,S,R,T),bf),V((2,T,Dm),bf),V((3,4,S,S,R,Q),bf),V((4,S,S,R,Q),bf),V((4,4,S,S,R,Q),bf),
            msg(4),msg(4),msg(4),msg(2),msg(2),msg(2),V((2,4,S,R,Q),f32),
            small(4),small(4),small(4),small(2),small(2),small(2),
            V((2,4,R,Q),bf),V((2,R,Dm),bf),V((2,R,Dm),f32),V((2,R,Dm),f32),V((2,R,Dm),bf),
            V((2,Dm,F),bf),V((TM,F),bf),V((TM,Dm),bf),V((TM,Dm),bf),V((TM,Dm),bf),V((2,TM,Dm//2),f32),V((2,TM,Dm//2),f32),
            DS((2,)),DS(()),DS((2+K,)),DS((3,)),DS((2,2)),DS((2,4)),DS((3,2)),DS((2,)),DS((2,2)),
            DS(()),DS((4,)),DS((10,2,4)),DS((10,4,4)),DS((2,)),DS((4,))],
        compiler_params=pltpu.CompilerParams(collective_id=0,has_side_effects=True,vmem_limit_bytes=67043328),name="mega",
    )(hv(hid1T),av(a1T),hv(hid0T),av(a0T),dy,dg1,du1,wg,wu,wd,s0,t0,h1,mg,mu,md,vg,vu,vd)
    return out

def final(wag,gsum,ms,vs):
    U,_,_,S,_,R,Q=wag.shape; n=2*S*S; Dm=4*Q; L=ms[0].shape[0]; K=U//(3*L)
    ms=(ms[0].reshape(L,K,R,Dm),*ms[1:]); vs=(vs[0].reshape(L,K,R,Dm),*vs[1:])
    B=2
    def kern(w_ref,g_ref,*refs):
        m,v,wo,mo,vo=(refs[3*i:3*i+3] for i in range(5))
        kind=div(B*pl.program_id(0),L*K)
        for t in range(3):
            @pl.when(kind==t)
            def _():
                for p in range(B):
                    for cc in range(2):
                        for r in range(S*S):
                            for q in range(4):
                                v_=w_ref[p,cc,q,r//S,r%S] if q<2 else w_ref[p,cc,q,r%S,r//S]
                                if t: wo[t][0,(2*r+cc)*R:(2*r+cc+1)*R,p*Dm+q*Q:p*Dm+q*Q+Q]=v_
                                else: wo[t][0,2*r+cc,p,:,q*Q:q*Q+Q]=v_
                    g=g_ref[p].astype(f32)
                    at=(0,slice(None),slice(p*Dm,p*Dm+Dm)) if t else (0,p)
                    mo[t][at]=0.9*m[t][at]+0.1*g
                    vo[t][at]=0.95*v[t][at]+0.05*g*g
    H=K//B; E=L*H
    def lk(s,t): s=jnp.clip(s-t*E,0,E-1); return div(s,H),rem(s,H)
    def unit(s): l,k=lk(rem(s,E),0); return ((L-1-l)*3+div(s,E))*H+k
    def spec(t,d,g):
        def at(s): l,k=lk(s,t); return (l,0,k) if t else (l,*[0]*(len(d)-4),k,0,0)
        return pl.BlockSpec(g if t else d,at)
    sd=jax.ShapeDtypeStruct
    mom=[spec(t,(1,B,R,Dm),(1,R,B*Dm)) for t in range(3)]
    o=pl.pallas_call(kern,grid=(U//B,),
        in_specs=[pl.BlockSpec((B,2,4,S,S,R,Q),lambda s:(unit(s),*[0]*6)),pl.BlockSpec((B,R,Dm),lambda s:(unit(s),0,0))]+mom*2,
        out_specs=[spec(t,(1,n,B,R,Dm),(1,Dm,B*Dm)) for t in range(3)]+mom*2,
        out_shape=[sd((L,n,K,R,Dm),bf),sd((L,Dm,K*Dm),bf),sd((L,Dm,K*Dm),bf)]+[sd(a.shape,f32) for a in (*ms,*vs)],
        name="final",compiler_params=pltpu.CompilerParams(vmem_limit_bytes=VM))(wag,gsum,*ms,*vs)
    w,m,v=o[:3],o[3:6],o[6:]
    order=lambda d,g,u: (g,u,d.reshape(L,-1,Dm))
    return (*order(*w),*order(*m),*order(*v))

def solution(mesh):
    from jax.sharding import PartitionSpec as P
    n=mesh.shape["dp"]
    def step(x,dy,wg,wu,wd,mg,mu,md,vg,vu,vd):
        x,dy=x[0],dy[0]
        hid0T,s0,t0,a0T,h1,a1,a1T=p01(x,wg,wu,wd)
        hid1T,dg1,du1=p2(a1,dy,wg,wu,wd,1)
        wag,gsum,_,_=mega(n,hid1T,a1T,hid0T,a0T,dy,dg1,du1,wg,wu,wd,s0,t0,h1,mg,mu,md,vg,vu,vd)
        return final(wag,gsum,(md,mg,mu),(vd,vg,vu))
    tok=P(("rep","dp"),None,None); w=P(None,None,None); m=P(None,"dp",None)
    return jax.shard_map(step,mesh=mesh,in_specs=(tok,tok,w,w,w)+(m,)*6,
        out_specs=(P("rep",None,None),)*3+(P("rep","dp",None),)*6,check_vma=False)
```
